16 devices in a mesh: dp: 2 (over y, z), ep: 8 (over x, core).
Axes of the slice: x: 4, y: 2, z: 1, core: 2. Of those that a mesh axis runs over, the one named last changes fastest.
The devices are a block of a 4x4x8 slice.
Arguments:
- x: bfloat16 [2, 8, 256, 2048], P('dp', 'ep'), parts along dimension 0
- expert: int32 [2, 8, 256, 2], P('dp', 'ep'), parts along dimension 0
- slot: int32 [2, 8, 256, 2], P('dp', 'ep'), parts along dimension 0
- gate: float32 [2, 8, 256, 2], P('dp', 'ep'), parts along dimension 0
- w_gate: bfloat16 [8, 2048, 5632], P('ep')
- w_up: bfloat16 [8, 2048, 5632], P('ep')
- w_down: bfloat16 [8, 5632, 2048], P('ep')
Outputs:
- y: bfloat16 [2, 8, 256, 2048], P('dp', 'ep'), parts along dimension 0
There are 2 independent parts. The reference program is written for one: setup_inputs(seed, part) draws one part's arguments, and reference() takes and returns one part's arrays. A program takes and returns all parts, laid end to end along the dimension named above; an argument that names none is the same for every part.
All inputs are finite; a program needn't handle non-finite values.
Results may differ from the reference program's by a relative error of at most 0.009.
Values are sent between devices in bfloat16 or wider.
A program may use at most 768 MiB of HBM per device.

```python
import jax
import jax.numpy as jnp

MEMBERS = 8
TOKENS = 256
D = 2048
FF = 5632
TOP = 2
EXPERTS = 8
SLOTS = 5 * TOKENS * TOP // (4 * EXPERTS)


def setup_inputs(seed: int = 0, part: int = 0) -> dict:
    own, k1, k2, k3, k4, k5, k6 = jax.random.split(jax.random.key(seed), 7)
    kx, ke, kl, kg = jax.random.split(jax.random.fold_in(own, part), 4)
    devices = (1, MEMBERS)
    place = jax.random.permutation(kl, jnp.arange(EXPERTS, dtype=jnp.uint32))
    slow = ((EXPERTS + (9 * place) % EXPERTS) << ((9 * place) // EXPERTS)) // EXPERTS
    wait = (jax.random.bits(ke, (*devices, TOKENS, EXPERTS), jnp.uint32) >> 10) * slow
    expert = jnp.argsort(wait, axis=-1)[..., :TOP].astype(jnp.int32)
    chosen = jax.nn.one_hot(expert, EXPERTS, dtype=jnp.int32)
    in_line = jnp.cumsum(chosen.reshape(*devices, TOKENS * TOP, EXPERTS), axis=2) - 1
    slot = jnp.sum(in_line.reshape(chosen.shape) * chosen, axis=-1)

    def one(key, rows, columns):
        return (jax.random.normal(key, (rows, columns), jnp.float32) * rows**-0.5).astype(jnp.bfloat16)

    def weights(key, rows, columns):
        return jax.lax.map(lambda k: one(k, rows, columns), jax.random.split(key, EXPERTS))

    return {
        "x": jax.random.normal(kx, (*devices, TOKENS, D), jnp.float32).astype(jnp.bfloat16),
        "expert": expert,
        "slot": slot,
        "gate": jax.nn.softmax(jax.random.normal(kg, expert.shape, jnp.float32)),
        "w_gate": weights(k1, D, FF),
        "w_up": weights(k2, D, FF),
        "w_down": weights(k3, FF, D),
    }


def einsum(form, a, b):
    return jnp.einsum(form, a.astype(jnp.float32), b.astype(jnp.float32))


def reference(x, expert, slot, gate, w_gate, w_up, w_down):
    to_expert = jax.nn.one_hot(expert, EXPERTS, dtype=jnp.bfloat16)
    to_slot = jax.nn.one_hot(slot, SLOTS, dtype=jnp.bfloat16)
    weighted = to_expert * gate[..., None].astype(jnp.bfloat16)
    dispatch = einsum("abtke,abtkc->abtec", to_expert, to_slot).astype(jnp.bfloat16)
    combine = einsum("abtke,abtkc->abtec", weighted, to_slot).astype(jnp.bfloat16)
    z = einsum("abtec,abtd->aebcd", dispatch, x).astype(jnp.bfloat16)
    h = jax.nn.silu(einsum("aebcd,edf->aebcf", z, w_gate))
    h = (h * einsum("aebcd,edf->aebcf", z, w_up)).astype(jnp.bfloat16)
    out = einsum("aebcf,efd->aebcd", h, w_down).astype(jnp.bfloat16)
    y = einsum("abtec,aebcd->abtd", combine, out)
    return y.astype(jnp.bfloat16)
```

```python
import functools

import jax
import jax.numpy as jnp
from jax import lax
from jax.experimental import pallas as pl
from jax.experimental.pallas import tpu as pltpu
from jax.sharding import PartitionSpec as P

MESH = pl.DeviceIdType.MESH
F_TILE = 512
D_TILE = 256
RING = 4
AHEAD = 3
SPLITS = ((0, 16, 48, 80), (0, 32, 64, 80), (0, 32, 48, 80))
FLIP = (0, 2, 1)
f32, bf16 = jnp.float32, jnp.bfloat16


def dot(a, b):
    return jnp.dot(a, b, preferred_element_type=f32)


def kernel(
    n_ep, slots,
    x_hbm, ex_ref, sl_ref, gt_ref, wg_hbm, wu_hbm, wd_hbm, y_hbm,
    z, zs, h, wg, wu, wd, comb,
    x_sem, g_sem, u_sem, d_sem, y_sem, out_send, out_recv, back_send, back_recv, free,
):
    tokens, dim = x_hbm.shape[2:]
    ff = h.shape[1]
    n_f, n_d = ff // F_TILE, dim // (2 * D_TILE)
    rows = h.shape[0]
    wide = 2 * D_TILE
    me = lax.axis_index("ep")
    chips = n_ep // 2
    chip, core = me // 2, lax.rem(me, 2)

    def peer(cls, c):
        step = (chips // 2, 1, chips - 1)[cls]
        return lax.rem(chip + step, chips) * 2 + c

    sibling = chip * 2 + 1 - core

    def load_f(i):
        cols = pl.ds(pl.multiple_of(i * F_TILE, F_TILE), F_TILE)
        return (
            pltpu.make_async_copy(wg_hbm.at[0, :, cols], wg.at[i], g_sem.at[i]),
            pltpu.make_async_copy(wu_hbm.at[0, :, cols], wu.at[i], u_sem.at[i]),
        )

    def load_d(block, slot):
        cols = pl.ds(pl.multiple_of(block * D_TILE, D_TILE), D_TILE)
        return pltpu.make_async_copy(wd_hbm.at[0, :, cols], wd.at[slot], d_sem.at[slot])

    def column(b):
        return pl.ds(pl.multiple_of(b * D_TILE, D_TILE), D_TILE)

    def strip(b):
        return pl.ds(pl.multiple_of(b * tokens, tokens), tokens)

    def get_x(b):
        return pltpu.make_async_copy(
            x_hbm.at[0, 0, :, column(b)], wd.at[RING - 1, strip(b)], x_sem.at[b]
        )

    for b in range(dim // D_TILE):
        get_x(b).start()
    for i in range(AHEAD):
        for c in load_f(i):
            c.start()

    barrier = pltpu.get_barrier_semaphore()
    for k in range(1, n_ep):
        pl.semaphore_signal(
            barrier, inc=1, device_id={"ep": lax.rem(me + k, n_ep)}, device_id_type=MESH
        )

    order = [me, sibling] + [peer(cls, c) for cls in range(3) for c in range(2)]
    top = ex_ref.shape[0]
    expert, slot_of = ex_ref[...], sl_ref[...]
    rank = functools.reduce(
        lambda v, r: jnp.where(expert == order[r], r, v), range(1, n_ep), jnp.zeros_like(expert)
    )
    key = jnp.where(slot_of < slots, rank * slots + slot_of, -1)

    def hit(start, size, k):
        at = start + lax.broadcasted_iota(jnp.int32, (size, tokens), 0)
        return key[k : k + 1, :] == at

    for p in range(n_ep // 2):
        hits = [hit(p * rows, rows, k) for k in range(top)]
        any_hit = functools.reduce(jnp.logical_or, hits)
        h[:, p * tokens : (p + 1) * tokens] = jnp.where(any_hit, 1.0, 0.0).astype(bf16)
    for b in range(dim // D_TILE):
        get_x(b).wait()

    def dispatch(b, _):
        tile = wd[RING - 1, strip(b), :]
        for p in reversed(range(n_ep // 2)):
            out = dot(h[:, p * tokens : (p + 1) * tokens], tile).astype(bf16)
            if p == 0:
                z[0:slots, column(b)] = out[0:slots]
                zs[slots:rows, column(b)] = out[slots:rows]
            else:
                zs[p * rows : (p + 1) * rows, column(b)] = out
        return 0

    lax.fori_loop(0, dim // D_TILE, dispatch, 0)

    def unit(g, cls, c):
        return ((g - 1) * 3 + cls) * 2 + c

    last = 6 * (len(SPLITS[0]) - 1)

    def place(g, cls, c):
        sizes = [SPLITS[q][g] - SPLITS[q][g - 1] for q in range(3)]
        return g * rows + 2 * sum(sizes[:cls]) + c * sizes[cls], sizes[cls]

    def home(g, cls, c):
        return (2 + 2 * cls + c) * slots + SPLITS[FLIP[cls]][g - 1]

    def go(g, cls, c):
        there, n = place(g, FLIP[cls], core)
        there = pl.multiple_of(there, 16)
        return pltpu.make_async_remote_copy(
            src_ref=zs.at[pl.ds(home(g, cls, c), n)],
            dst_ref=z.at[pl.ds(there, n)],
            send_sem=out_send.at[unit(g, cls, c)],
            recv_sem=out_recv.at[unit(g, FLIP[cls], core)],
            device_id={"ep": peer(cls, c)},
            device_id_type=MESH,
        )

    def come(g, cls, c):
        here, n = place(g, cls, c)
        return pltpu.make_async_remote_copy(
            src_ref=zs.at[pl.ds(0, n)],
            dst_ref=z.at[pl.ds(here, n)],
            send_sem=out_send.at[unit(g, cls, c)],
            recv_sem=out_recv.at[unit(g, cls, c)],
            device_id={"ep": peer(cls, c)},
            device_id_type=MESH,
        )

    go_sib = pltpu.make_async_remote_copy(
        src_ref=zs.at[pl.ds(slots, slots)],
        dst_ref=z.at[pl.ds(slots, slots)],
        send_sem=out_send.at[last],
        recv_sem=out_recv.at[last],
        device_id={"ep": sibling},
        device_id_type=MESH,
    )
    passes = range(1, len(SPLITS[0]))
    peers = [(cls, c) for cls in range(3) for c in range(2)]
    near = [(1, 0), (2, 0), (1, 1), (2, 1), (0, 0), (0, 1)]

    pl.semaphore_wait(barrier, n_ep - 1)
    go_sib.start()
    for g in passes:
        for cls, c in near:
            go(g, cls, c).start()

    gates = gt_ref[...].astype(bf16).astype(f32)
    for start in range(0, n_ep * slots, 128):
        part = jnp.zeros((128, tokens), f32)
        for k in range(top):
            part = part + jnp.where(hit(start, 128, k), gates[k : k + 1, :], 0.0)
        comb[:, start : start + 128] = part.T.astype(bf16)

    def back(g, cls, c, j):
        here, n = place(g, cls, c)
        there = pl.multiple_of(
            (2 + 2 * FLIP[cls] + core) * slots + SPLITS[cls][g - 1], 16
        )
        cols = pl.ds(pl.multiple_of(j * wide, wide), wide)
        return pltpu.make_async_remote_copy(
            src_ref=z.at[pl.ds(here, n), cols],
            dst_ref=zs.at[pl.ds(there, n), cols],
            send_sem=back_send.at[unit(g, cls, c), j],
            recv_sem=back_recv.at[unit(g, FLIP[cls], core), j],
            device_id={"ep": peer(cls, c)},
            device_id_type=MESH,
        )

    def back_here(g, cls, c, j):
        here = home(g, cls, c)
        n = place(g, FLIP[cls], 0)[1]
        cols = pl.ds(pl.multiple_of(j * wide, wide), wide)
        return pltpu.make_async_remote_copy(
            src_ref=z.at[pl.ds(0, n), cols],
            dst_ref=zs.at[pl.ds(here, n), cols],
            send_sem=back_send.at[unit(g, cls, c), j],
            recv_sem=back_recv.at[unit(g, cls, c), j],
            device_id={"ep": peer(cls, c)},
            device_id_type=MESH,
        )

    def back_sib(j):
        cols = pl.ds(pl.multiple_of(j * wide, wide), wide)
        return pltpu.make_async_remote_copy(
            src_ref=z.at[pl.ds(slots, slots), cols],
            dst_ref=zs.at[pl.ds(slots, slots), cols],
            send_sem=back_send.at[last, j],
            recv_sem=back_recv.at[last, j],
            device_id={"ep": sibling},
            device_id_type=MESH,
        )

    n_pass = len(SPLITS[0])
    blocks = 2 * n_d

    for g in range(n_pass):
        first = g * rows
        if g == 0:
            go_sib.wait()
            pl.semaphore_signal(
                free.at[last], inc=1, device_id={"ep": sibling}, device_id_type=MESH
            )
        else:
            for cls, c in peers:
                come(g, cls, c).wait_recv()
                go(g, cls, c).wait_send()
                pl.semaphore_signal(
                    free.at[unit(g, FLIP[cls], core)],
                    inc=1,
                    device_id={"ep": peer(cls, c)},
                    device_id_type=MESH,
                )

        def gate_up(i, _):
            if g == 0:
                for c in load_f(i):
                    c.wait()

                @pl.when(i + AHEAD < n_f)
                def _():
                    for c in load_f(i + AHEAD):
                        c.start()

                @pl.when(jnp.logical_and(i + AHEAD >= n_f, i + AHEAD < n_f + RING))
                def _():
                    q = i + AHEAD - n_f
                    load_d(q, q).start()

            rows_in = z[first : first + rows, :]
            a = dot(rows_in, wg[i])
            b = dot(rows_in, wu[i])
            cols = pl.ds(pl.multiple_of(i * F_TILE, F_TILE), F_TILE)
            h[:, cols] = (a * jax.nn.sigmoid(a) * b).astype(bf16)
            return 0

        lax.fori_loop(0, n_f, gate_up, 0)
        if g == 0:
            for q in range(AHEAD, RING):
                load_d(q, q).start()

        def down(j, _):
            for s in range(2):
                q = 2 * j + s
                slot = lax.rem(q, RING)
                load_d(q, slot).wait()
            q0 = lax.rem(2 * j, RING)
            a = dot(h[...], wd[q0])
            b = dot(h[...], wd[q0 + 1])
            col = pl.multiple_of(j * wide, wide)
            z[first : first + rows, pl.ds(col, D_TILE)] = a.astype(bf16)
            z[first : first + rows, pl.ds(col + D_TILE, D_TILE)] = b.astype(bf16)
            if g == 0:
                zs[0:slots, pl.ds(col, D_TILE)] = a[0:slots].astype(bf16)
                zs[0:slots, pl.ds(col + D_TILE, D_TILE)] = b[0:slots].astype(bf16)

            def refill():
                for s in range(2):
                    q = 2 * j + s + RING
                    load_d(lax.rem(q, blocks), lax.rem(q, RING)).start()

            if g < n_pass - 1:
                refill()
            else:
                pl.when(2 * j + RING < blocks)(refill)
            if g == 0:
                back_sib(j).start()
            else:
                for cls, c in near:
                    back(g, cls, c, j).start()
            return 0

        if g == 0:
            pl.semaphore_wait(free.at[last], 1)
        else:
            for cls, c in peers:
                pl.semaphore_wait(free.at[unit(g, cls, c)], 1)
        lax.fori_loop(0, n_d, down, 0)

    def put(b):
        return pltpu.make_async_copy(
            wd.at[0, strip(b)], y_hbm.at[0, 0, :, column(b)], y_sem.at[b]
        )

    def combine(j, _):
        back_sib(j).wait()
        for g in passes:
            for cls, c in peers:
                back_here(g, cls, c, j).wait_recv()
                back(g, cls, c, j).wait_send()
        for s in range(2):
            b = 2 * j + s
            wd[0, strip(b), :] = dot(comb[...], zs[:, column(b)]).astype(bf16)
            put(b).start()
        return 0

    lax.fori_loop(0, n_d, combine, 0)
    for b in range(2 * n_d):
        put(b).wait()


def solution(mesh):
    n_ep = mesh.shape["ep"]

    def local(x, expert, slot, gate, w_gate, w_up, w_down):
        tokens, dim = x.shape[2:]
        top, ff = expert.shape[3], w_gate.shape[2]
        slots = 5 * tokens * top // (4 * n_ep)
        rows = 2 * slots
        n_d = dim // (2 * D_TILE)
        units = 6 * (len(SPLITS[0]) - 1) + 1
        dma = pltpu.SemaphoreType.DMA
        hbm = pl.BlockSpec(memory_space=pltpu.MemorySpace.HBM)
        vmem = pl.BlockSpec(memory_space=pltpu.VMEM)
        return pl.pallas_call(
            functools.partial(kernel, n_ep, slots),
            out_shape=jax.ShapeDtypeStruct(x.shape, x.dtype),
            in_specs=[hbm, vmem, vmem, vmem, hbm, hbm, hbm],
            out_specs=hbm,
            scratch_shapes=[
                pltpu.VMEM((n_ep * slots, dim), bf16),
                pltpu.VMEM((n_ep * slots, dim), bf16),
                pltpu.VMEM((rows, ff), bf16),
                pltpu.VMEM((ff // F_TILE, dim, F_TILE), bf16),
                pltpu.VMEM((ff // F_TILE, dim, F_TILE), bf16),
                pltpu.VMEM((RING, ff, D_TILE), bf16),
                pltpu.VMEM((tokens, n_ep * slots), bf16),
                dma((dim // D_TILE,)),
                dma((ff // F_TILE,)),
                dma((ff // F_TILE,)),
                dma((RING,)),
                dma((dim // D_TILE,)),
                dma((units,)),
                dma((units,)),
                dma((units, n_d)),
                dma((units, n_d)),
                pltpu.SemaphoreType.REGULAR((units,)),
            ],
            compiler_params=pltpu.CompilerParams(
                collective_id=0, has_side_effects=True, vmem_limit_bytes=67_043_328
            ),
        )(
            x,
            expert.reshape(tokens, top).T,
            slot.reshape(tokens, top).T,
            gate.reshape(tokens, top).T,
            w_gate,
            w_up,
            w_down,
        )

    act, wt = P("dp", "ep", None, None), P("ep", None, None)
    return jax.shard_map(
        local, mesh=mesh, in_specs=(act,) * 4 + (wt,) * 3, out_specs=act, check_vma=False
    )
```

```python
import functools

import jax
import jax.numpy as jnp
from jax import lax
from jax.experimental import pallas as pl
from jax.experimental.pallas import tpu as pltpu
from jax.sharding import PartitionSpec as P

MESH = pl.DeviceIdType.MESH
F_TILE = 512
D_TILE = 256
RING = 3
AHEAD = 3
SPLITS = ((0, 16, 48, 80), (0, 32, 64, 80), (0, 32, 48, 80))
FLIP = (0, 2, 1)
f32, bf16 = jnp.float32, jnp.bfloat16


def dot(a, b):
    return jnp.dot(a, b, preferred_element_type=f32)


def kernel(
    n_ep, slots,
    x_hbm, ex_ref, sl_ref, gt_ref, wg_hbm, wu_hbm, wd_hbm, y_hbm,
    z, zs, h, wg, wu, wd, comb,
    x_sem, g_sem, u_sem, d_sem, y_sem, out_send, out_recv, back_send, back_recv, free,
):
    tokens, dim = x_hbm.shape[2:]
    ff = h.shape[2]
    n_f, n_d = ff // F_TILE, dim // D_TILE
    rows = h.shape[1]
    wide = D_TILE
    me = lax.axis_index("ep")
    chips = n_ep // 2
    chip, core = me // 2, lax.rem(me, 2)

    def peer(cls, c):
        step = (chips // 2, 1, chips - 1)[cls]
        return lax.rem(chip + step, chips) * 2 + c

    sibling = chip * 2 + 1 - core

    def load_f(i):
        cols = pl.ds(pl.multiple_of(i * F_TILE, F_TILE), F_TILE)
        return (
            pltpu.make_async_copy(wg_hbm.at[0, :, cols], wg.at[i], g_sem.at[i]),
            pltpu.make_async_copy(wu_hbm.at[0, :, cols], wu.at[i], u_sem.at[i]),
        )

    def load_d(block, slot):
        cols = pl.ds(pl.multiple_of(block * D_TILE, D_TILE), D_TILE)
        return pltpu.make_async_copy(wd_hbm.at[0, :, cols], wd.at[slot], d_sem.at[slot])

    def column(b):
        return pl.ds(pl.multiple_of(b * D_TILE, D_TILE), D_TILE)

    def strip(b):
        return pl.ds(pl.multiple_of(b * tokens, tokens), tokens)

    def get_x(b):
        return pltpu.make_async_copy(
            x_hbm.at[0, 0, :, column(b)], wd.at[RING - 1, strip(b)], x_sem.at[b]
        )

    for b in range(dim // D_TILE):
        get_x(b).start()
    for i in range(AHEAD):
        for c in load_f(i):
            c.start()

    barrier = pltpu.get_barrier_semaphore()
    for k in range(1, n_ep):
        pl.semaphore_signal(
            barrier, inc=1, device_id={"ep": lax.rem(me + k, n_ep)}, device_id_type=MESH
        )

    order = [me, sibling] + [peer(cls, c) for cls in range(3) for c in range(2)]
    top = ex_ref.shape[0]
    expert, slot_of = ex_ref[...], sl_ref[...]
    rank = functools.reduce(
        lambda v, r: jnp.where(expert == order[r], r, v), range(1, n_ep), jnp.zeros_like(expert)
    )
    key = jnp.where(slot_of < slots, rank * slots + slot_of, -1)

    def hit(start, size, k):
        at = start + lax.broadcasted_iota(jnp.int32, (size, tokens), 0)
        return key[k : k + 1, :] == at

    for p in range(n_ep // 2):
        hits = [hit(p * rows, rows, k) for k in range(top)]
        any_hit = functools.reduce(jnp.logical_or, hits)
        h[0, :, p * tokens : (p + 1) * tokens] = jnp.where(any_hit, 1.0, 0.0).astype(bf16)
    for b in range(dim // D_TILE):
        get_x(b).wait()

    def dispatch(b, _):
        tile = wd[RING - 1, strip(b), :]
        for p in reversed(range(n_ep // 2)):
            out = dot(h[0, :, p * tokens : (p + 1) * tokens], tile).astype(bf16)
            if p == 0:
                z[0:slots, column(b)] = out[0:slots]
                zs[slots:rows, column(b)] = out[slots:rows]
            else:
                zs[p * rows : (p + 1) * rows, column(b)] = out
        return 0

    lax.fori_loop(0, dim // D_TILE, dispatch, 0)

    def unit(g, cls, c):
        return ((g - 1) * 3 + cls) * 2 + c

    last = 6 * (len(SPLITS[0]) - 1)

    def place(g, cls, c):
        sizes = [SPLITS[q][g] - SPLITS[q][g - 1] for q in range(3)]
        return g * rows + 2 * sum(sizes[:cls]) + c * sizes[cls], sizes[cls]

    def home(g, cls, c):
        return (2 + 2 * cls + c) * slots + SPLITS[FLIP[cls]][g - 1]

    def go(g, cls, c):
        there, n = place(g, FLIP[cls], core)
        there = pl.multiple_of(there, 16)
        return pltpu.make_async_remote_copy(
            src_ref=zs.at[pl.ds(home(g, cls, c), n)],
            dst_ref=z.at[pl.ds(there, n)],
            send_sem=out_send.at[unit(g, cls, c)],
            recv_sem=out_recv.at[unit(g, FLIP[cls], core)],
            device_id={"ep": peer(cls, c)},
            device_id_type=MESH,
        )

    def come(g, cls, c):
        here, n = place(g, cls, c)
        return pltpu.make_async_remote_copy(
            src_ref=zs.at[pl.ds(0, n)],
            dst_ref=z.at[pl.ds(here, n)],
            send_sem=out_send.at[unit(g, cls, c)],
            recv_sem=out_recv.at[unit(g, cls, c)],
            device_id={"ep": peer(cls, c)},
            device_id_type=MESH,
        )

    go_sib = pltpu.make_async_remote_copy(
        src_ref=zs.at[pl.ds(slots, slots)],
        dst_ref=z.at[pl.ds(slots, slots)],
        send_sem=out_send.at[last],
        recv_sem=out_recv.at[last],
        device_id={"ep": sibling},
        device_id_type=MESH,
    )
    passes = range(1, len(SPLITS[0]))
    peers = [(cls, c) for cls in range(3) for c in range(2)]
    near = [(1, 0), (2, 0), (1, 1), (2, 1), (0, 0), (0, 1)]

    pl.semaphore_wait(barrier, n_ep - 1)
    go_sib.start()
    for g in passes:
        for cls, c in near:
            go(g, cls, c).start()

    gates = gt_ref[...].astype(bf16).astype(f32)
    for start in range(0, n_ep * slots, 128):
        part = jnp.zeros((128, tokens), f32)
        for k in range(top):
            part = part + jnp.where(hit(start, 128, k), gates[k : k + 1, :], 0.0)
        comb[:, start : start + 128] = part.T.astype(bf16)

    def back(g, cls, c, j):
        here, n = place(g, cls, c)
        there = pl.multiple_of(
            (2 + 2 * FLIP[cls] + core) * slots + SPLITS[cls][g - 1], 16
        )
        cols = pl.ds(pl.multiple_of(j * wide, wide), wide)
        return pltpu.make_async_remote_copy(
            src_ref=z.at[pl.ds(here, n), cols],
            dst_ref=zs.at[pl.ds(there, n), cols],
            send_sem=back_send.at[unit(g, cls, c), j],
            recv_sem=back_recv.at[unit(g, FLIP[cls], core), j],
            device_id={"ep": peer(cls, c)},
            device_id_type=MESH,
        )

    def back_here(g, cls, c, j):
        here = home(g, cls, c)
        n = place(g, FLIP[cls], 0)[1]
        cols = pl.ds(pl.multiple_of(j * wide, wide), wide)
        return pltpu.make_async_remote_copy(
            src_ref=z.at[pl.ds(0, n), cols],
            dst_ref=zs.at[pl.ds(here, n), cols],
            send_sem=back_send.at[unit(g, cls, c), j],
            recv_sem=back_recv.at[unit(g, cls, c), j],
            device_id={"ep": peer(cls, c)},
            device_id_type=MESH,
        )

    def back_sib(j):
        cols = pl.ds(pl.multiple_of(j * wide, wide), wide)
        return pltpu.make_async_remote_copy(
            src_ref=z.at[pl.ds(slots, slots), cols],
            dst_ref=zs.at[pl.ds(slots, slots), cols],
            send_sem=back_send.at[last, j],
            recv_sem=back_recv.at[last, j],
            device_id={"ep": sibling},
            device_id_type=MESH,
        )

    def gather(g):
        if g == 0:
            go_sib.wait()
            pl.semaphore_signal(
                free.at[last], inc=1, device_id={"ep": sibling}, device_id_type=MESH
            )
        else:
            for cls, c in peers:
                come(g, cls, c).wait_recv()
                go(g, cls, c).wait_send()
                pl.semaphore_signal(
                    free.at[unit(g, FLIP[cls], core)],
                    inc=1,
                    device_id={"ep": peer(cls, c)},
                    device_id_type=MESH,
                )

    def expand(g, to):
        gather(g)

        def gate_up(i, _):
            if g == 0:
                for c in load_f(i):
                    c.wait()

                @pl.when(i + AHEAD < n_f)
                def _():
                    for c in load_f(i + AHEAD):
                        c.start()

                @pl.when(i + AHEAD >= n_f)
                def _():
                    q = i + AHEAD - n_f
                    load_d(q, q).start()

            rows_in = z[g * rows : (g + 1) * rows, :]
            a = dot(rows_in, wg[i])
            b = dot(rows_in, wu[i])
            cols = pl.ds(pl.multiple_of(i * F_TILE, F_TILE), F_TILE)
            h[to, :, cols] = (a * jax.nn.sigmoid(a) * b).astype(bf16)
            return 0

        lax.fori_loop(0, n_f, gate_up, 0)

    def contract(pair, start, more):
        for g, _ in pair:
            if g == 0:
                pl.semaphore_wait(free.at[last], 1)
            else:
                for cls, c in peers:
                    pl.semaphore_wait(free.at[unit(g, cls, c)], 1)

        def down(j, _):
            q = start + j
            slot = lax.rem(q, RING)
            load_d(j, slot).wait()
            outs = [dot(h[at], wd[slot]).astype(bf16) for _, at in pair]
            for (g, _), out in zip(pair, outs):
                z[g * rows : (g + 1) * rows, column(j)] = out
                if g == 0:
                    zs[0:slots, column(j)] = out[0:slots]

            def refill():
                load_d(lax.rem(j + RING, n_d), slot).start()

            if more:
                refill()
            else:
                pl.when(j + RING < n_d)(refill)
            for g, _ in pair:
                if g == 0:
                    back_sib(j).start()
                else:
                    for cls, c in near:
                        back(g, cls, c, j).start()
            return 0

        lax.fori_loop(0, n_d, down, 0)

    expand(0, 2)
    expand(1, 0)
    expand(2, 1)
    contract(((1, 0), (2, 1)), 0, True)
    expand(3, 0)
    contract(((3, 0), (0, 2)), n_d, False)

    def put(b):
        return pltpu.make_async_copy(
            wd.at[0, strip(b)], y_hbm.at[0, 0, :, column(b)], y_sem.at[b]
        )

    def combine(j, _):
        back_sib(j).wait()
        for g in passes:
            for cls, c in peers:
                back_here(g, cls, c, j).wait_recv()
                back(g, cls, c, j).wait_send()
        wd[0, strip(j), :] = dot(comb[...], zs[:, column(j)]).astype(bf16)
        put(j).start()
        return 0

    lax.fori_loop(0, n_d, combine, 0)
    for b in range(n_d):
        put(b).wait()


def solution(mesh):
    n_ep = mesh.shape["ep"]

    def local(x, expert, slot, gate, w_gate, w_up, w_down):
        tokens, dim = x.shape[2:]
        top, ff = expert.shape[3], w_gate.shape[2]
        slots = 5 * tokens * top // (4 * n_ep)
        rows = 2 * slots
        n_d = dim // D_TILE
        units = 6 * (len(SPLITS[0]) - 1) + 1
        dma = pltpu.SemaphoreType.DMA
        hbm = pl.BlockSpec(memory_space=pltpu.MemorySpace.HBM)
        vmem = pl.BlockSpec(memory_space=pltpu.VMEM)
        return pl.pallas_call(
            functools.partial(kernel, n_ep, slots),
            out_shape=jax.ShapeDtypeStruct(x.shape, x.dtype),
            in_specs=[hbm, vmem, vmem, vmem, hbm, hbm, hbm],
            out_specs=hbm,
            scratch_shapes=[
                pltpu.VMEM((n_ep * slots, dim), bf16),
                pltpu.VMEM((n_ep * slots, dim), bf16),
                pltpu.VMEM((3, rows, ff), bf16),
                pltpu.VMEM((ff // F_TILE, dim, F_TILE), bf16),
                pltpu.VMEM((ff // F_TILE, dim, F_TILE), bf16),
                pltpu.VMEM((RING, ff, D_TILE), bf16),
                pltpu.VMEM((tokens, n_ep * slots), bf16),
                dma((dim // D_TILE,)),
                dma((ff // F_TILE,)),
                dma((ff // F_TILE,)),
                dma((RING,)),
                dma((dim // D_TILE,)),
                dma((units,)),
                dma((units,)),
                dma((units, n_d)),
                dma((units, n_d)),
                pltpu.SemaphoreType.REGULAR((units,)),
            ],
            compiler_params=pltpu.CompilerParams(
                collective_id=0, has_side_effects=True, vmem_limit_bytes=67_043_328
            ),
        )(
            x,
            expert.reshape(tokens, top).T,
            slot.reshape(tokens, top).T,
            gate.reshape(tokens, top).T,
            w_gate,
            w_up,
            w_down,
        )

    act, wt = P("dp", "ep", None, None), P("ep", None, None)
    return jax.shard_map(
        local, mesh=mesh, in_specs=(act,) * 4 + (wt,) * 3, out_specs=act, check_vma=False
    )
```

```python
import functools

import jax
import jax.numpy as jnp
from jax import lax
from jax.experimental import pallas as pl
from jax.experimental.pallas import tpu as pltpu
from jax.sharding import PartitionSpec as P

MESH = pl.DeviceIdType.MESH
F_TILE = 512
D_TILE = 256
RING = 3
AHEAD = 3
SPLITS = ((0, 16, 48, 80), (0, 32, 64, 80), (0, 32, 48, 80))
FLIP = (0, 2, 1)
f32, bf16 = jnp.float32, jnp.bfloat16


def dot(a, b):
    return jnp.dot(a, b, preferred_element_type=f32)


def kernel(
    n_ep, slots,
    x_hbm, ex_ref, sl_ref, gt_ref, wg_hbm, wu_hbm, wd_hbm, y_hbm,
    z, zs, h, wf, wd, comb,
    x_sem, f_sem, d_sem, y_sem, out_send, out_recv, back_send, back_recv, free,
):
    tokens, dim = x_hbm.shape[2:]
    ff = h.shape[2]
    n_f, n_d = ff // F_TILE, dim // D_TILE
    rows = h.shape[1]
    wide = D_TILE
    me = lax.axis_index("ep")
    chips = n_ep // 2
    chip, core = me // 2, lax.rem(me, 2)

    def peer(cls, c):
        step = (chips // 2, 1, chips - 1)[cls]
        return lax.rem(chip + step, chips) * 2 + c

    sibling = chip * 2 + 1 - core

    def load_f(i):
        cols = pl.ds(pl.multiple_of(i * F_TILE, F_TILE), F_TILE)
        sem = f_sem.at[lax.rem(i, AHEAD)]
        return (
            pltpu.make_async_copy(wg_hbm.at[0, :, cols], wf.at[i, 0], sem),
            pltpu.make_async_copy(wu_hbm.at[0, :, cols], wf.at[i, 1], sem),
        )

    def load_d(block, slot):
        cols = pl.ds(pl.multiple_of(block * D_TILE, D_TILE), D_TILE)
        return pltpu.make_async_copy(wd_hbm.at[0, :, cols], wd.at[slot], d_sem.at[slot])

    def column(b):
        return pl.ds(pl.multiple_of(b * D_TILE, D_TILE), D_TILE)

    def strip(b):
        return pl.ds(pl.multiple_of(b * tokens, tokens), tokens)

    def get_x(b):
        return pltpu.make_async_copy(
            x_hbm.at[0, 0, :, column(b)], wd.at[RING - 1, strip(b)], x_sem
        )

    for b in range(dim // D_TILE):
        get_x(b).start()
    for i in range(AHEAD):
        for c in load_f(i):
            c.start()

    barrier = pltpu.get_barrier_semaphore()
    for k in range(1, n_ep):
        pl.semaphore_signal(
            barrier, inc=1, device_id={"ep": lax.rem(me + k, n_ep)}, device_id_type=MESH
        )

    order = [me, sibling] + [peer(cls, c) for cls in range(3) for c in range(2)]
    top = ex_ref.shape[0]
    expert, slot_of = ex_ref[...], sl_ref[...]
    rank = functools.reduce(
        lambda v, r: jnp.where(expert == order[r], r, v), range(1, n_ep), jnp.zeros_like(expert)
    )
    key = jnp.where(slot_of < slots, rank * slots + slot_of, -1)

    def hit(start, size, k):
        at = start + lax.broadcasted_iota(jnp.int32, (size, tokens), 0)
        return key[k : k + 1, :] == at

    for p in range(n_ep // 2):
        hits = [hit(p * rows, rows, k) for k in range(top)]
        any_hit = functools.reduce(jnp.logical_or, hits)
        h[0, :, p * tokens : (p + 1) * tokens] = jnp.where(any_hit, 1.0, 0.0).astype(bf16)
    whole = wd.at[RING - 1, pl.ds(0, dim // D_TILE * tokens)]
    pltpu.make_async_copy(whole, whole, x_sem).wait()

    def dispatch(b, _):
        tile = wd[RING - 1, strip(b), :]
        for p in reversed(range(n_ep // 2)):
            out = dot(h[0, :, p * tokens : (p + 1) * tokens], tile).astype(bf16)
            if p == 0:
                z[0:slots, column(b)] = out[0:slots]
                zs[slots:rows, column(b)] = out[slots:rows]
            else:
                zs[p * rows : (p + 1) * rows, column(b)] = out
        return 0

    lax.fori_loop(0, dim // D_TILE, dispatch, 0)

    def place(g, cls, c):
        sizes = [SPLITS[q][g] - SPLITS[q][g - 1] for q in range(3)]
        return g * rows + 2 * sum(sizes[:cls]) + c * sizes[cls], sizes[cls]

    def home(g, cls, c):
        return (2 + 2 * cls + c) * slots + SPLITS[FLIP[cls]][g - 1]

    def go(g, cls, c):
        there, n = place(g, FLIP[cls], core)
        there = pl.multiple_of(there, 16)
        return pltpu.make_async_remote_copy(
            src_ref=zs.at[pl.ds(home(g, cls, c), n)],
            dst_ref=z.at[pl.ds(there, n)],
            send_sem=out_send.at[g],
            recv_sem=out_recv.at[g],
            device_id={"ep": peer(cls, c)},
            device_id_type=MESH,
        )

    def arrived(g):
        to = z.at[pl.ds(g * rows, rows)]
        return (
            pltpu.make_async_copy(to, to, out_recv.at[g]),
            pltpu.make_async_copy(to, to, out_send.at[g]),
        )

    go_sib = pltpu.make_async_remote_copy(
        src_ref=zs.at[pl.ds(slots, slots)],
        dst_ref=z.at[pl.ds(slots, slots)],
        send_sem=out_send.at[0],
        recv_sem=out_recv.at[0],
        device_id={"ep": sibling},
        device_id_type=MESH,
    )
    passes = range(1, len(SPLITS[0]))
    peers = [(cls, c) for cls in range(3) for c in range(2)]
    near = [(1, 0), (2, 0), (1, 1), (2, 1), (0, 0), (0, 1)]

    pl.semaphore_wait(barrier, n_ep - 1)
    go_sib.start()
    for g in passes:
        for cls, c in near:
            go(g, cls, c).start()

    gates = gt_ref[...].astype(bf16).astype(f32)
    for start in range(0, n_ep * slots, 128):
        part = jnp.zeros((128, tokens), f32)
        for k in range(top):
            part = part + jnp.where(hit(start, 128, k), gates[k : k + 1, :], 0.0)
        comb[:, start : start + 128] = part.T.astype(bf16)

    def back(g, cls, c, j):
        here, n = place(g, cls, c)
        there = pl.multiple_of(
            (2 + 2 * FLIP[cls] + core) * slots + SPLITS[cls][g - 1], 16
        )
        cols = pl.ds(pl.multiple_of(j * wide, wide), wide)
        return pltpu.make_async_remote_copy(
            src_ref=z.at[pl.ds(here, n), cols],
            dst_ref=zs.at[pl.ds(there, n), cols],
            send_sem=back_send,
            recv_sem=back_recv.at[j],
            device_id={"ep": peer(cls, c)},
            device_id_type=MESH,
        )

    def back_sib(j):
        cols = pl.ds(pl.multiple_of(j * wide, wide), wide)
        return pltpu.make_async_remote_copy(
            src_ref=z.at[pl.ds(slots, slots), cols],
            dst_ref=zs.at[pl.ds(slots, slots), cols],
            send_sem=back_send,
            recv_sem=back_recv.at[j],
            device_id={"ep": sibling},
            device_id_type=MESH,
        )

    def gather(g):
        if g == 0:
            go_sib.wait()
            pl.semaphore_signal(
                free.at[0], inc=1, device_id={"ep": sibling}, device_id_type=MESH
            )
        else:
            for c in arrived(g):
                c.wait()
            for cls, c in peers:
                pl.semaphore_signal(
                    free.at[g], inc=1, device_id={"ep": peer(cls, c)}, device_id_type=MESH
                )

    def expand(g, to):
        gather(g)

        def gate_up(i, _):
            if g == 0:
                pltpu.make_async_copy(wf.at[i], wf.at[i], f_sem.at[lax.rem(i, AHEAD)]).wait()

                @pl.when(i + AHEAD < n_f)
                def _():
                    for c in load_f(i + AHEAD):
                        c.start()

                @pl.when(i + AHEAD >= n_f)
                def _():
                    q = i + AHEAD - n_f
                    load_d(q, q).start()

            rows_in = z[g * rows : (g + 1) * rows, :]
            a = dot(rows_in, wf[i, 0])
            b = dot(rows_in, wf[i, 1])
            cols = pl.ds(pl.multiple_of(i * F_TILE, F_TILE), F_TILE)
            h[to, :, cols] = (a * jax.nn.sigmoid(a) * b).astype(bf16)
            return 0

        if g == 0:
            lax.fori_loop(0, n_f, gate_up, 0)
        else:
            for i in range(n_f):
                gate_up(i, 0)

    def contract(pair, start, more):
        for g, _ in pair:
            pl.semaphore_wait(free.at[g], 1 if g == 0 else len(peers))

        def down(j, _):
            q = start + j
            slot = lax.rem(q, RING)
            load_d(j, slot).wait()
            outs = [dot(h[at], wd[slot]).astype(bf16) for _, at in pair]
            for (g, _), out in zip(pair, outs):
                z[g * rows : (g + 1) * rows, column(j)] = out
                if g == 0:
                    zs[0:slots, column(j)] = out[0:slots]

            def refill():
                load_d(lax.rem(j + RING, n_d), slot).start()

            if more:
                refill()
            else:
                pl.when(j + RING < n_d)(refill)
            for g, _ in pair:
                if g == 0:
                    back_sib(j).start()
                else:
                    for cls, c in near:
                        back(g, cls, c, j).start()
            return 0

        lax.fori_loop(0, n_d, down, 0)

    expand(0, 2)
    expand(1, 0)
    expand(2, 1)
    contract(((1, 0), (2, 1)), 0, True)
    expand(3, 0)
    contract(((3, 0), (0, 2)), n_d, False)

    def put(b):
        return pltpu.make_async_copy(
            wd.at[0, strip(b)], y_hbm.at[0, 0, :, column(b)], y_sem
        )

    def combine(j, _):
        strip_in = zs.at[pl.ds(slots, (n_ep - 1) * slots), column(j)]
        pltpu.make_async_copy(strip_in, strip_in, back_recv.at[j]).wait()
        wd[0, strip(j), :] = dot(comb[...], zs[:, column(j)]).astype(bf16)
        put(j).start()
        return 0

    lax.fori_loop(0, n_d, combine, 0)
    sent = z.at[pl.ds(slots, (n_ep - 1) * slots)]
    pltpu.make_async_copy(sent, sent, back_send).wait()
    whole = wd.at[0, pl.ds(0, n_d * tokens)]
    pltpu.make_async_copy(whole, whole, y_sem).wait()


def solution(mesh):
    n_ep = mesh.shape["ep"]

    def local(x, expert, slot, gate, w_gate, w_up, w_down):
        tokens, dim = x.shape[2:]
        top, ff = expert.shape[3], w_gate.shape[2]
        slots = 5 * tokens * top // (4 * n_ep)
        rows = 2 * slots
        n_d = dim // D_TILE
        n_pass = len(SPLITS[0])
        dma = pltpu.SemaphoreType.DMA
        hbm = pl.BlockSpec(memory_space=pltpu.MemorySpace.HBM)
        vmem = pl.BlockSpec(memory_space=pltpu.VMEM)
        return pl.pallas_call(
            functools.partial(kernel, n_ep, slots),
            out_shape=jax.ShapeDtypeStruct(x.shape, x.dtype),
            in_specs=[hbm, vmem, vmem, vmem, hbm, hbm, hbm],
            out_specs=hbm,
            scratch_shapes=[
                pltpu.VMEM((n_ep * slots, dim), bf16),
                pltpu.VMEM((n_ep * slots, dim), bf16),
                pltpu.VMEM((3, rows, ff), bf16),
                pltpu.VMEM((ff // F_TILE, 2, dim, F_TILE), bf16),
                pltpu.VMEM((RING, ff, D_TILE), bf16),
                pltpu.VMEM((tokens, n_ep * slots), bf16),
                dma(()),
                dma((AHEAD,)),
                dma((RING,)),
                dma(()),
                dma((n_pass,)),
                dma((n_pass,)),
                dma(()),
                dma((n_d,)),
                pltpu.SemaphoreType.REGULAR((n_pass,)),
            ],
            compiler_params=pltpu.CompilerParams(
                collective_id=0, has_side_effects=True, vmem_limit_bytes=67_043_328
            ),
        )(
            x,
            expert.reshape(tokens, top).T,
            slot.reshape(tokens, top).T,
            gate.reshape(tokens, top).T,
            w_gate,
            w_up,
            w_down,
        )

    act, wt = P("dp", "ep", None, None), P("ep", None, None)
    return jax.shard_map(
        local, mesh=mesh, in_specs=(act,) * 4 + (wt,) * 3, out_specs=act, check_vma=False
    )
```

```python
import functools

import jax
import jax.numpy as jnp
from jax import lax
from jax.experimental import pallas as pl
from jax.experimental.pallas import tpu as pltpu
from jax.sharding import PartitionSpec as P

MESH = pl.DeviceIdType.MESH
F_TILE = 512
D_TILE = 256
RING = 3
AHEAD = 3
SPLITS = ((0, 16, 48, 80), (0, 32, 64, 80), (0, 32, 48, 80))
FLIP = (0, 2, 1)
f32, bf16 = jnp.float32, jnp.bfloat16


def dot(a, b):
    return jnp.dot(a, b, preferred_element_type=f32)


def kernel(
    n_ep, slots,
    x_hbm, ex_ref, sl_ref, gt_ref, wg_hbm, wu_hbm, wd_hbm, y_hbm,
    z, zs, h, wf, wd, comb,
    x_sem, f_sem, d_sem, y_sem, out_send, out_recv, back_send, back_recv, free,
):
    tokens, dim = x_hbm.shape[2:]
    ff = h.shape[2]
    n_f, n_d = ff // F_TILE, dim // D_TILE
    rows = h.shape[1]
    wide = D_TILE
    me = lax.axis_index("ep")
    chips = n_ep // 2
    chip, core = me // 2, lax.rem(me, 2)

    def peer(cls, c):
        step = (chips // 2, 1, chips - 1)[cls]
        return lax.rem(chip + step, chips) * 2 + c

    sibling = chip * 2 + 1 - core

    def load_f(i):
        cols = pl.ds(pl.multiple_of(i * F_TILE, F_TILE), F_TILE)
        sem = f_sem.at[lax.rem(i, AHEAD)]
        return (
            pltpu.make_async_copy(wg_hbm.at[0, :, cols], wf.at[i, 0], sem),
            pltpu.make_async_copy(wu_hbm.at[0, :, cols], wf.at[i, 1], sem),
        )

    def load_d(block, slot):
        cols = pl.ds(pl.multiple_of(block * D_TILE, D_TILE), D_TILE)
        return pltpu.make_async_copy(wd_hbm.at[0, :, cols], wd.at[slot], d_sem.at[slot])

    barrier = pltpu.get_barrier_semaphore()
    for k in range(1, n_ep):
        pl.semaphore_signal(
            barrier, inc=1, device_id={"ep": lax.rem(me + k, n_ep)}, device_id_type=MESH
        )

    def column(b):
        return pl.ds(pl.multiple_of(b * D_TILE, D_TILE), D_TILE)

    def strip(b):
        return pl.ds(pl.multiple_of(b * tokens, tokens), tokens)

    def get_x(b):
        return pltpu.make_async_copy(
            x_hbm.at[0, 0, :, column(b)], wd.at[RING - 1, strip(b)], x_sem
        )

    for b in range(dim // D_TILE):
        get_x(b).start()

    order = [me, sibling] + [peer(cls, c) for cls in range(3) for c in range(2)]
    top = ex_ref.shape[0]
    expert, slot_of = ex_ref[...], sl_ref[...]
    rank = functools.reduce(
        lambda v, r: jnp.where(expert == order[r], r, v), range(1, n_ep), jnp.zeros_like(expert)
    )
    key = jnp.where(slot_of < slots, rank * slots + slot_of, -1)

    def hit(start, size, k):
        at = start + lax.broadcasted_iota(jnp.int32, (size, tokens), 0)
        return key[k : k + 1, :] == at

    for p in range(n_ep // 2):
        hits = [hit(p * rows, rows, k) for k in range(top)]
        any_hit = functools.reduce(jnp.logical_or, hits)
        h[0, :, p * tokens : (p + 1) * tokens] = jnp.where(any_hit, 1.0, 0.0).astype(bf16)
    gates = gt_ref[...].astype(bf16).astype(f32)
    for start in range(0, n_ep * slots, 128):
        part = jnp.zeros((128, tokens), f32)
        for k in range(top):
            part = part + jnp.where(hit(start, 128, k), gates[k : k + 1, :], 0.0)
        comb[:, start : start + 128] = part.T.astype(bf16)

    whole = wd.at[RING - 1, pl.ds(0, dim // D_TILE * tokens)]
    pltpu.make_async_copy(whole, whole, x_sem).wait()
    for i in range(AHEAD):
        for c in load_f(i):
            c.start()

    def dispatch(p):
        for b in range(dim // D_TILE):
            tile = wd[RING - 1, strip(b), :]
            out = dot(h[0, :, p * tokens : (p + 1) * tokens], tile).astype(bf16)
            if p == 0:
                z[0:slots, column(b)] = out[0:slots]
                zs[slots:rows, column(b)] = out[slots:rows]
            else:
                zs[p * rows : (p + 1) * rows, column(b)] = out

    dispatch(2)
    dispatch(3)

    def place(g, cls, c):
        sizes = [SPLITS[q][g] - SPLITS[q][g - 1] for q in range(3)]
        return g * rows + 2 * sum(sizes[:cls]) + c * sizes[cls], sizes[cls]

    def home(g, cls, c):
        return (2 + 2 * cls + c) * slots + SPLITS[FLIP[cls]][g - 1]

    def go(g, cls, c):
        there, n = place(g, FLIP[cls], core)
        there = pl.multiple_of(there, 16)
        return pltpu.make_async_remote_copy(
            src_ref=zs.at[pl.ds(home(g, cls, c), n)],
            dst_ref=z.at[pl.ds(there, n)],
            send_sem=out_send.at[g],
            recv_sem=out_recv.at[g],
            device_id={"ep": peer(cls, c)},
            device_id_type=MESH,
        )

    def arrived(g):
        to = z.at[pl.ds(g * rows, rows)]
        return (
            pltpu.make_async_copy(to, to, out_recv.at[g]),
            pltpu.make_async_copy(to, to, out_send.at[g]),
        )

    go_sib = pltpu.make_async_remote_copy(
        src_ref=zs.at[pl.ds(slots, slots)],
        dst_ref=z.at[pl.ds(slots, slots)],
        send_sem=out_send.at[0],
        recv_sem=out_recv.at[0],
        device_id={"ep": sibling},
        device_id_type=MESH,
    )
    passes = range(1, len(SPLITS[0]))
    peers = [(cls, c) for cls in range(3) for c in range(2)]
    near = [(1, 0), (2, 0), (1, 1), (2, 1), (0, 0), (0, 1)]

    pl.semaphore_wait(barrier, n_ep - 1)
    for cls, c in near[:4]:
        go(1, cls, c).start()
    dispatch(1)
    for cls, c in near[4:]:
        go(1, cls, c).start()
    for g in passes[1:]:
        for cls, c in near:
            go(g, cls, c).start()
    dispatch(0)
    go_sib.start()

    def back(g, cls, c, j):
        here, n = place(g, cls, c)
        there = pl.multiple_of(
            (2 + 2 * FLIP[cls] + core) * slots + SPLITS[cls][g - 1], 16
        )
        cols = pl.ds(pl.multiple_of(j * wide, wide), wide)
        return pltpu.make_async_remote_copy(
            src_ref=z.at[pl.ds(here, n), cols],
            dst_ref=zs.at[pl.ds(there, n), cols],
            send_sem=back_send,
            recv_sem=back_recv.at[j],
            device_id={"ep": peer(cls, c)},
            device_id_type=MESH,
        )

    def back_sib(j):
        cols = pl.ds(pl.multiple_of(j * wide, wide), wide)
        return pltpu.make_async_remote_copy(
            src_ref=z.at[pl.ds(slots, slots), cols],
            dst_ref=zs.at[pl.ds(slots, slots), cols],
            send_sem=back_send,
            recv_sem=back_recv.at[j],
            device_id={"ep": sibling},
            device_id_type=MESH,
        )

    def gather(g):
        if g == 0:
            go_sib.wait()
            pl.semaphore_signal(
                free.at[0], inc=1, device_id={"ep": sibling}, device_id_type=MESH
            )
        else:
            for c in arrived(g):
                c.wait()
            for cls, c in peers:
                pl.semaphore_signal(
                    free.at[g], inc=1, device_id={"ep": peer(cls, c)}, device_id_type=MESH
                )

    def expand(g, to):
        gather(g)

        def gate_up(i, _):
            if g == 0:
                pltpu.make_async_copy(wf.at[i], wf.at[i], f_sem.at[lax.rem(i, AHEAD)]).wait()

                @pl.when(i + AHEAD < n_f)
                def _():
                    for c in load_f(i + AHEAD):
                        c.start()

                @pl.when(i + AHEAD >= n_f)
                def _():
                    q = i + AHEAD - n_f
                    load_d(q, q).start()

            rows_in = z[g * rows : (g + 1) * rows, :]
            a = dot(rows_in, wf[i, 0])
            b = dot(rows_in, wf[i, 1])
            cols = pl.ds(pl.multiple_of(i * F_TILE, F_TILE), F_TILE)
            h[to, :, cols] = (a * jax.nn.sigmoid(a) * b).astype(bf16)
            return 0

        if g == 0:
            lax.fori_loop(0, n_f, gate_up, 0)
        else:
            for i in range(n_f):
                gate_up(i, 0)

    def contract(pair, start, more):
        for g, _ in pair:
            pl.semaphore_wait(free.at[g], 1 if g == 0 else len(peers))

        def down(j, _):
            q = start + j
            slot = lax.rem(q, RING)
            load_d(j, slot).wait()
            outs = [dot(h[at], wd[slot]).astype(bf16) for _, at in pair]
            for (g, _), out in zip(pair, outs):
                z[g * rows : (g + 1) * rows, column(j)] = out
                if g == 0:
                    zs[0:slots, column(j)] = out[0:slots]

            def refill():
                load_d(lax.rem(j + RING, n_d), slot).start()

            if more:
                refill()
            else:
                pl.when(j + RING < n_d)(refill)
            for g, _ in pair:
                if g == 0:
                    back_sib(j).start()
                else:
                    for cls, c in near:
                        back(g, cls, c, j).start()
            return 0

        lax.fori_loop(0, n_d, down, 0)

    expand(0, 2)
    expand(1, 0)
    expand(2, 1)
    contract(((1, 0), (2, 1)), 0, True)
    expand(3, 0)
    contract(((3, 0), (0, 2)), n_d, False)

    def put(b):
        return pltpu.make_async_copy(
            wd.at[0, strip(b)], y_hbm.at[0, 0, :, column(b)], y_sem
        )

    def combine(j, _):
        strip_in = zs.at[pl.ds(slots, (n_ep - 1) * slots), column(j)]
        pltpu.make_async_copy(strip_in, strip_in, back_recv.at[j]).wait()
        wd[0, strip(j), :] = dot(comb[...], zs[:, column(j)]).astype(bf16)
        put(j).start()
        return 0

    lax.fori_loop(0, n_d, combine, 0)
    sent = z.at[pl.ds(slots, (n_ep - 1) * slots)]
    pltpu.make_async_copy(sent, sent, back_send).wait()
    whole = wd.at[0, pl.ds(0, n_d * tokens)]
    pltpu.make_async_copy(whole, whole, y_sem).wait()


def solution(mesh):
    n_ep = mesh.shape["ep"]

    def local(x, expert, slot, gate, w_gate, w_up, w_down):
        tokens, dim = x.shape[2:]
        top, ff = expert.shape[3], w_gate.shape[2]
        slots = 5 * tokens * top // (4 * n_ep)
        rows = 2 * slots
        n_d = dim // D_TILE
        n_pass = len(SPLITS[0])
        dma = pltpu.SemaphoreType.DMA
        hbm = pl.BlockSpec(memory_space=pltpu.MemorySpace.HBM)
        vmem = pl.BlockSpec(memory_space=pltpu.VMEM)
        return pl.pallas_call(
            functools.partial(kernel, n_ep, slots),
            out_shape=jax.ShapeDtypeStruct(x.shape, x.dtype),
            in_specs=[hbm, vmem, vmem, vmem, hbm, hbm, hbm],
            out_specs=hbm,
            scratch_shapes=[
                pltpu.VMEM((n_ep * slots, dim), bf16),
                pltpu.VMEM((n_ep * slots, dim), bf16),
                pltpu.VMEM((3, rows, ff), bf16),
                pltpu.VMEM((ff // F_TILE, 2, dim, F_TILE), bf16),
                pltpu.VMEM((RING, ff, D_TILE), bf16),
                pltpu.VMEM((tokens, n_ep * slots), bf16),
                dma(()),
                dma((AHEAD,)),
                dma((RING,)),
                dma(()),
                dma((n_pass,)),
                dma((n_pass,)),
                dma(()),
                dma((n_d,)),
                pltpu.SemaphoreType.REGULAR((n_pass,)),
            ],
            compiler_params=pltpu.CompilerParams(
                collective_id=0, has_side_effects=True, vmem_limit_bytes=67_043_328
            ),
        )(
            x,
            expert.reshape(tokens, top).T,
            slot.reshape(tokens, top).T,
            gate.reshape(tokens, top).T,
            w_gate,
            w_up,
            w_down,
        )

    act, wt = P("dp", "ep", None, None), P("ep", None, None)
    return jax.shard_map(
        local, mesh=mesh, in_specs=(act,) * 4 + (wt,) * 3, out_specs=act, check_vma=False
    )
```

```python
import functools

import jax
import jax.numpy as jnp
from jax import lax
from jax.experimental import pallas as pl
from jax.experimental.pallas import tpu as pltpu
from jax.sharding import PartitionSpec as P

MESH = pl.DeviceIdType.MESH
F_TILE = 512
D_TILE = 256
RING = 3
AHEAD = 3
SPLITS = ((0, 16, 48, 80), (0, 32, 64, 80), (0, 32, 48, 80))
FLIP = (0, 2, 1)
f32, bf16 = jnp.float32, jnp.bfloat16


def dot(a, b):
    return jnp.dot(a, b, preferred_element_type=f32)


def kernel(
    n_ep, slots,
    x_hbm, ex_ref, sl_ref, gt_ref, wg_hbm, wu_hbm, wd_hbm, y_hbm,
    z, zs, h, wf, wd, comb,
    x_sem, f_sem, d_sem, y_sem, out_send, out_recv, back_send, back_recv, free,
):
    tokens, dim = x_hbm.shape[2:]
    ff = h.shape[2]
    n_f, n_d = ff // F_TILE, dim // D_TILE
    rows = h.shape[1]
    wide = D_TILE
    me = lax.axis_index("ep")
    chips = n_ep // 2
    chip, core = me // 2, lax.rem(me, 2)

    def peer(cls, c):
        step = (chips // 2, 1, chips - 1)[cls]
        return lax.rem(chip + step, chips) * 2 + c

    sibling = chip * 2 + 1 - core

    def load_f(i):
        cols = pl.ds(pl.multiple_of(i * F_TILE, F_TILE), F_TILE)
        sem = f_sem.at[lax.rem(i, AHEAD)]
        return (
            pltpu.make_async_copy(wg_hbm.at[0, :, cols], wf.at[i, 0], sem),
            pltpu.make_async_copy(wu_hbm.at[0, :, cols], wf.at[i, 1], sem),
        )

    def load_d(block, slot):
        cols = pl.ds(pl.multiple_of(block * D_TILE, D_TILE), D_TILE)
        return pltpu.make_async_copy(wd_hbm.at[0, :, cols], wd.at[slot], d_sem.at[slot])

    barrier = pltpu.get_barrier_semaphore()
    for k in range(1, n_ep):
        pl.semaphore_signal(
            barrier, inc=1, device_id={"ep": lax.rem(me + k, n_ep)}, device_id_type=MESH
        )

    def column(b):
        return pl.ds(pl.multiple_of(b * D_TILE, D_TILE), D_TILE)

    def strip(b):
        return pl.ds(pl.multiple_of(b * tokens, tokens), tokens)

    def get_x(b):
        return pltpu.make_async_copy(
            x_hbm.at[0, 0, :, column(b)], wd.at[RING - 1, strip(b)], x_sem
        )

    for b in range(dim // D_TILE):
        get_x(b).start()
    for i in range(AHEAD):
        for c in load_f(i):
            c.start(priority=1)

    order = [me, sibling] + [peer(cls, c) for cls in range(3) for c in range(2)]
    top = ex_ref.shape[0]
    expert, slot_of = ex_ref[...], sl_ref[...]
    rank = functools.reduce(
        lambda v, r: jnp.where(expert == order[r], r, v), range(1, n_ep), jnp.zeros_like(expert)
    )
    key = jnp.where(slot_of < slots, rank * slots + slot_of, -1)

    def hit(start, size, k):
        at = start + lax.broadcasted_iota(jnp.int32, (size, tokens), 0)
        return key[k : k + 1, :] == at

    for p in range(n_ep // 2):
        hits = [hit(p * rows, rows, k) for k in range(top)]
        any_hit = functools.reduce(jnp.logical_or, hits)
        h[0, :, p * tokens : (p + 1) * tokens] = jnp.where(any_hit, 1.0, 0.0).astype(bf16)
    gates = gt_ref[...].astype(bf16).astype(f32)
    for start in range(0, n_ep * slots, 128):
        part = jnp.zeros((128, tokens), f32)
        for k in range(top):
            part = part + jnp.where(hit(start, 128, k), gates[k : k + 1, :], 0.0)
        comb[:, start : start + 128] = part.T.astype(bf16)

    whole = wd.at[RING - 1, pl.ds(0, dim // D_TILE * tokens)]
    pltpu.make_async_copy(whole, whole, x_sem).wait()

    def dispatch(p):
        for b in range(dim // D_TILE):
            tile = wd[RING - 1, strip(b), :]
            out = dot(h[0, :, p * tokens : (p + 1) * tokens], tile).astype(bf16)
            if p == 0:
                z[0:slots, column(b)] = out[0:slots]
                zs[slots:rows, column(b)] = out[slots:rows]
            else:
                zs[p * rows : (p + 1) * rows, column(b)] = out

    dispatch(2)
    dispatch(3)

    def place(g, cls, c):
        sizes = [SPLITS[q][g] - SPLITS[q][g - 1] for q in range(3)]
        return g * rows + 2 * sum(sizes[:cls]) + c * sizes[cls], sizes[cls]

    def home(g, cls, c):
        return (2 + 2 * cls + c) * slots + SPLITS[FLIP[cls]][g - 1]

    def go(g, cls, c):
        there, n = place(g, FLIP[cls], core)
        there = pl.multiple_of(there, 16)
        return pltpu.make_async_remote_copy(
            src_ref=zs.at[pl.ds(home(g, cls, c), n)],
            dst_ref=z.at[pl.ds(there, n)],
            send_sem=out_send.at[g],
            recv_sem=out_recv.at[g],
            device_id={"ep": peer(cls, c)},
            device_id_type=MESH,
        )

    def arrived(g):
        to = z.at[pl.ds(g * rows, rows)]
        return (
            pltpu.make_async_copy(to, to, out_recv.at[g]),
            pltpu.make_async_copy(to, to, out_send.at[g]),
        )

    go_sib = pltpu.make_async_remote_copy(
        src_ref=zs.at[pl.ds(slots, slots)],
        dst_ref=z.at[pl.ds(slots, slots)],
        send_sem=out_send.at[0],
        recv_sem=out_recv.at[0],
        device_id={"ep": sibling},
        device_id_type=MESH,
    )
    passes = range(1, len(SPLITS[0]))
    peers = [(cls, c) for cls in range(3) for c in range(2)]
    near = [(1, 0), (2, 0), (1, 1), (2, 1), (0, 0), (0, 1)]

    pl.semaphore_wait(barrier, n_ep - 1)
    for cls, c in near[:4]:
        go(1, cls, c).start()
    dispatch(1)
    for cls, c in near[4:]:
        go(1, cls, c).start()
    for g in passes[1:]:
        for cls, c in near:
            go(g, cls, c).start()
    dispatch(0)
    go_sib.start()

    def back(g, cls, c, j):
        here, n = place(g, cls, c)
        there = pl.multiple_of(
            (2 + 2 * FLIP[cls] + core) * slots + SPLITS[cls][g - 1], 16
        )
        cols = pl.ds(pl.multiple_of(j * wide, wide), wide)
        return pltpu.make_async_remote_copy(
            src_ref=z.at[pl.ds(here, n), cols],
            dst_ref=zs.at[pl.ds(there, n), cols],
            send_sem=back_send,
            recv_sem=back_recv.at[j],
            device_id={"ep": peer(cls, c)},
            device_id_type=MESH,
        )

    def back_sib(j):
        cols = pl.ds(pl.multiple_of(j * wide, wide), wide)
        return pltpu.make_async_remote_copy(
            src_ref=z.at[pl.ds(slots, slots), cols],
            dst_ref=zs.at[pl.ds(slots, slots), cols],
            send_sem=back_send,
            recv_sem=back_recv.at[j],
            device_id={"ep": sibling},
            device_id_type=MESH,
        )

    def gather(g):
        if g == 0:
            go_sib.wait()
            pl.semaphore_signal(
                free.at[0], inc=1, device_id={"ep": sibling}, device_id_type=MESH
            )
        else:
            for c in arrived(g):
                c.wait()
            for cls, c in peers:
                pl.semaphore_signal(
                    free.at[g], inc=1, device_id={"ep": peer(cls, c)}, device_id_type=MESH
                )

    def expand(g, to):
        gather(g)

        def gate_up(i, _):
            if g == 0:
                pltpu.make_async_copy(wf.at[i], wf.at[i], f_sem.at[lax.rem(i, AHEAD)]).wait()

                @pl.when(i + AHEAD < n_f)
                def _():
                    for c in load_f(i + AHEAD):
                        c.start()

                @pl.when(i + AHEAD >= n_f)
                def _():
                    q = i + AHEAD - n_f
                    load_d(q, q).start()

            rows_in = z[g * rows : (g + 1) * rows, :]
            a = dot(rows_in, wf[i, 0])
            b = dot(rows_in, wf[i, 1])
            cols = pl.ds(pl.multiple_of(i * F_TILE, F_TILE), F_TILE)
            h[to, :, cols] = (a * jax.nn.sigmoid(a) * b).astype(bf16)
            return 0

        if g == 0:
            lax.fori_loop(0, n_f, gate_up, 0)
        else:
            for i in range(n_f):
                gate_up(i, 0)

    def contract(pair, start, more):
        for g, _ in pair:
            pl.semaphore_wait(free.at[g], 1 if g == 0 else len(peers))

        def down(j, _):
            q = start + j
            slot = lax.rem(q, RING)
            load_d(j, slot).wait()
            outs = [dot(h[at], wd[slot]).astype(bf16) for _, at in pair]
            for (g, _), out in zip(pair, outs):
                z[g * rows : (g + 1) * rows, column(j)] = out
                if g == 0:
                    zs[0:slots, column(j)] = out[0:slots]

            def refill():
                load_d(lax.rem(j + RING, n_d), slot).start()

            if more:
                refill()
            else:
                pl.when(j + RING < n_d)(refill)
            for g, _ in pair:
                if g == 0:
                    back_sib(j).start()
                else:
                    for cls, c in near:
                        back(g, cls, c, j).start()
            return 0

        lax.fori_loop(0, n_d, down, 0)

    expand(0, 2)
    expand(1, 0)
    expand(2, 1)
    contract(((1, 0), (2, 1)), 0, True)
    expand(3, 0)
    contract(((3, 0), (0, 2)), n_d, False)

    def put(b):
        return pltpu.make_async_copy(
            wd.at[0, strip(b)], y_hbm.at[0, 0, :, column(b)], y_sem
        )

    def combine(j, _):
        strip_in = zs.at[pl.ds(slots, (n_ep - 1) * slots), column(j)]
        pltpu.make_async_copy(strip_in, strip_in, back_recv.at[j]).wait()
        wd[0, strip(j), :] = dot(comb[...], zs[:, column(j)]).astype(bf16)
        put(j).start()
        return 0

    lax.fori_loop(0, n_d, combine, 0)
    sent = z.at[pl.ds(slots, (n_ep - 1) * slots)]
    pltpu.make_async_copy(sent, sent, back_send).wait()
    whole = wd.at[0, pl.ds(0, n_d * tokens)]
    pltpu.make_async_copy(whole, whole, y_sem).wait()


def carry(parts, y_in, y_out, held, in_sem, out_sem):
    size = held.shape[0] // parts
    ins = [
        pltpu.make_async_copy(
            y_in.at[0, 0, pl.ds(p * size, size)], held.at[pl.ds(p * size, size)], in_sem.at[p]
        )
        for p in range(parts)
    ]
    for c in ins:
        c.start()
    for p, c in enumerate(ins):
        c.wait()
        rows = pl.ds(p * size, size)
        pltpu.make_async_copy(held.at[rows], y_out.at[0, 0, rows], out_sem).start()
    pltpu.make_async_copy(held, held, out_sem).wait()


def solution(mesh):
    n_ep = mesh.shape["ep"]

    def local(x, expert, slot, gate, w_gate, w_up, w_down):
        tokens, dim = x.shape[2:]
        top, ff = expert.shape[3], w_gate.shape[2]
        slots = 5 * tokens * top // (4 * n_ep)
        rows = 2 * slots
        n_d = dim // D_TILE
        n_pass = len(SPLITS[0])
        dma = pltpu.SemaphoreType.DMA
        hbm = pl.BlockSpec(memory_space=pltpu.MemorySpace.HBM)
        vmem = pl.BlockSpec(memory_space=pltpu.VMEM)
        result = pl.pallas_call(
            functools.partial(kernel, n_ep, slots),
            out_shape=jax.ShapeDtypeStruct(x.shape, x.dtype),
            in_specs=[hbm, vmem, vmem, vmem, hbm, hbm, hbm],
            out_specs=hbm,
            scratch_shapes=[
                pltpu.VMEM((n_ep * slots, dim), bf16),
                pltpu.VMEM((n_ep * slots, dim), bf16),
                pltpu.VMEM((3, rows, ff), bf16),
                pltpu.VMEM((ff // F_TILE, 2, dim, F_TILE), bf16),
                pltpu.VMEM((RING, ff, D_TILE), bf16),
                pltpu.VMEM((tokens, n_ep * slots), bf16),
                dma(()),
                dma((AHEAD,)),
                dma((RING,)),
                dma(()),
                dma((n_pass,)),
                dma((n_pass,)),
                dma(()),
                dma((n_d,)),
                pltpu.SemaphoreType.REGULAR((n_pass,)),
            ],
            compiler_params=pltpu.CompilerParams(
                collective_id=0, has_side_effects=True, vmem_limit_bytes=67_043_328
            ),
        )(
            x,
            expert.reshape(tokens, top).T,
            slot.reshape(tokens, top).T,
            gate.reshape(tokens, top).T,
            w_gate,
            w_up,
            w_down,
        )
        parts = 4
        return pl.pallas_call(
            functools.partial(carry, parts),
            out_shape=jax.ShapeDtypeStruct(x.shape, x.dtype),
            in_specs=[hbm],
            out_specs=hbm,
            scratch_shapes=[
                pltpu.VMEM((tokens, dim), bf16),
                dma((parts,)),
                dma(()),
            ],
        )(result)

    act, wt = P("dp", "ep", None, None), P("ep", None, None)
    return jax.shard_map(
        local, mesh=mesh, in_specs=(act,) * 4 + (wt,) * 3, out_specs=act, check_vma=False
    )
```
